1024 devices in a mesh: island: 32 (over x_hi, z), tp: 32 (over y, x_lo, core).
Axes of the slice: x: 8 (x_hi: 4, x_lo: 2; x = x_hi * 2 + x_lo), y: 8, z: 8, core: 2. Of those that a mesh axis runs over, the one named last changes fastest.
Arguments:
- residual: bfloat16 [32, 256, 4096], P('island', 'tp'), may hold values from -4 to 4
- gate_pre: bfloat16 [32, 256, 7168], P('island', None, 'tp'), may hold values from -9 to 9
- up_pre: bfloat16 [32, 256, 7168], P('island', None, 'tp'), may hold values from -9 to 9
- down_weight: bfloat16 [7168, 4096], P('tp'), may hold values from -0.0625 to 0.0625
- cotangent: bfloat16 [32, 256, 4096], P('island', 'tp'), may hold values from -1.5 to 1.5
- outer_weights: float32 [32, 262144], P('island', 'tp'), may hold values from -6 to 6
- deltas: float32 [32, 262144], P('island', 'tp'), may hold values from -6 to 6
- momentum: float32 [32, 262144], P('island', 'tp'), may hold values from -6 to 6
- partner: int32 [32], replicated, may hold values from 0 to 31, as said below
Outputs:
- mixed: bfloat16 [32, 256, 4096], P('island', 'tp')
- grad_gate: bfloat16 [32, 256, 7168], P('island', None, 'tp')
- grad_up: bfloat16 [32, 256, 7168], P('island', None, 'tp')
- grad_down: bfloat16 [32, 7168, 4096], P('island', 'tp')
- new_outer: float32 [32, 262144], P('island', 'tp')
- new_momentum: float32 [32, 262144], P('island', 'tp')
The draws below stay inside these ranges and needn't reach their ends.
Inputs may be any that keep to these rules, and one draw needn't show every extreme that they name: Islands come in pairs: partner[partner[i]] = i and partner[i] != i for every island i.
All inputs are finite; a program needn't handle non-finite values.
Results may differ from the reference program's by a relative error of at most 0.023.
Values may be sent and summed in bfloat16 or wider, within the bound.
A program may use at most 32 MiB of HBM per device.

```python
import jax
import jax.numpy as jnp
from jax import lax

D = 4096
FF = 7168
TOK = 256
FRAG = 262144
ISLANDS = 32
N_TP = 32


def draw_partner(key, part):
    order = jax.random.permutation(jax.random.fold_in(key, 17), ISLANDS).astype(jnp.int32)
    firsts = order[0::2]
    seconds = order[1::2]
    table = jnp.zeros((ISLANDS,), jnp.int32)
    table = table.at[firsts].set(seconds)
    table = table.at[seconds].set(firsts)
    return table


def block_scale(key, extent, pieces, smallest, largest):
    loudness = 1.0
    for axis_at, parts in pieces:
        draws = jax.random.uniform(jax.random.fold_in(jax.random.fold_in(key, 6), axis_at), (parts,), jnp.float32, smallest / len(pieces), largest / len(pieces))
        loudness = loudness * jnp.repeat(jnp.exp(draws), extent[axis_at] // parts).reshape((-1,) + (1,) * (len(extent) - 1 - axis_at))
    return loudness


def scatter_about(rng, extent, deviation, limit, split=(), held_as=jnp.bfloat16):
    array = deviation * jax.random.normal(rng, extent, jnp.float32)
    if split:
        array = array * block_scale(rng, extent, split, -0.22, 0.18)
    return jnp.clip(array, -limit, limit).astype(held_as)


def setup_inputs(seed: int = 0) -> dict:
    arg_keys = jax.random.split(jax.random.key(seed), 10)
    return {
        "residual": scatter_about(arg_keys[0], (ISLANDS, TOK, D), 0.5, 4.0, ((0, 32), (1, 32))),
        "gate_pre": scatter_about(arg_keys[1], (ISLANDS, TOK, FF), 1.5, 9.0, ((0, 32), (2, 32))),
        "up_pre": scatter_about(arg_keys[2], (ISLANDS, TOK, FF), 1.5, 9.0, ((0, 32), (2, 32))),
        "down_weight": scatter_about(arg_keys[3], (FF, D), FF ** -0.5, 0.0625, ((0, 32),)),
        "cotangent": scatter_about(arg_keys[4], (ISLANDS, TOK, D), 0.25, 1.5, ((0, 32), (1, 32))),
        "outer_weights": scatter_about(arg_keys[5], (ISLANDS, FRAG), 1.0, 6.0, ((0, 32), (1, 32)), jnp.float32),
        "deltas": scatter_about(arg_keys[6], (ISLANDS, FRAG), 1.0, 6.0, ((0, 32), (1, 32)), jnp.float32),
        "momentum": scatter_about(arg_keys[7], (ISLANDS, FRAG), 1.0, 6.0, ((0, 32), (1, 32)), jnp.float32),
        "partner": draw_partner(jax.random.fold_in(arg_keys[9], 71), 0),
    }


decay_rate = 0.5
delta_rate = 0.7
pull_rate = 0.6


def island_layer(down_weight, inputs):
    residual, gate_pre, up_pre, cotangent = inputs
    gate_value = gate_pre.astype(jnp.float32)
    up_value = up_pre.astype(jnp.float32)
    logistic = jax.nn.sigmoid(gate_value)
    activated = gate_value * logistic
    hidden = (activated * up_value).astype(jnp.bfloat16)
    width = FF // N_TP
    hidden_blocks = hidden.reshape(TOK, N_TP, width).transpose(1, 0, 2)
    weight_blocks = down_weight.reshape(N_TP, width, D)

    def add_block(total, pair):
        block_hidden, block_weight = pair
        part = jnp.dot(block_hidden, block_weight, preferred_element_type=jnp.float32).astype(jnp.bfloat16)
        return total + part.astype(jnp.float32), None

    summed, _ = lax.scan(add_block, jnp.zeros((TOK, D), jnp.float32), (hidden_blocks, weight_blocks))
    mixed = (residual.astype(jnp.float32) + summed).astype(jnp.bfloat16)
    grad_down = jnp.dot(hidden.T, cotangent, preferred_element_type=jnp.float32).astype(jnp.bfloat16)
    grad_hidden = jnp.dot(cotangent, down_weight.T, preferred_element_type=jnp.float32)
    slope = logistic * (1.0 + gate_value * (1.0 - logistic))
    grad_gate = (grad_hidden * up_value * slope).astype(jnp.bfloat16)
    grad_up = (grad_hidden * activated).astype(jnp.bfloat16)
    return mixed, grad_gate, grad_up, grad_down


def reference(residual, gate_pre, up_pre, down_weight, cotangent, outer_weights, deltas, momentum, partner):
    mixed, grad_gate, grad_up, grad_down = lax.map(partial_layer(down_weight), (residual, gate_pre, up_pre, cotangent))
    partner_outer = outer_weights[partner.astype(jnp.int32)]
    partner_delta = deltas[partner.astype(jnp.int32)]
    new_momentum = decay_rate * momentum + 0.5 * delta_rate * (deltas + partner_delta) - 0.5 * pull_rate * (outer_weights - partner_outer)
    new_outer = outer_weights + new_momentum
    return mixed, grad_gate, grad_up, grad_down, new_outer, new_momentum


def partial_layer(down_weight):
    def apply_layer(inputs):
        return island_layer(down_weight, inputs)
    return apply_layer
```

```python
import functools

import jax
import jax.numpy as jnp
from jax import lax
from jax.experimental import pallas as pl
from jax.experimental.pallas import tpu as pltpu
from jax.sharding import Mesh
from jax.sharding import PartitionSpec as P

MESH = pl.DeviceIdType.MESH
ISLAND = ("xh", "z")
TP = ("y", "xl", "c")

decay_rate = 0.5
delta_rate = 0.7
pull_rate = 0.6

F32 = jnp.float32
BF16 = jnp.bfloat16

RIGHT, LEFT = 0, 1
F_A, F_B, P_A = 0, 1, 2


class Links:
    def __init__(self, send_sem, recv_sem):
        self.send_sem, self.recv_sem = send_sem, recv_sem
        self.numbers, self.sent = {}, []

    def number(self, key):
        return self.numbers.setdefault(key, len(self.numbers))

    def make(self, key, src, dst, peer):
        k = self.number(key)
        return pltpu.make_async_remote_copy(
            src_ref=src,
            dst_ref=dst,
            send_sem=self.send_sem.at[k],
            recv_sem=self.recv_sem.at[k],
            device_id=peer,
            device_id_type=MESH,
        )

    def send(self, key, src, dst, peer):
        copy = self.make(key, src, dst, peer)
        copy.start()
        self.sent.append(copy)

    def arrive(self, key, dst, peer):
        self.make(key, dst, dst, peer).wait_recv()

    def drain(self):
        for copy in self.sent:
            copy.wait_send()


def message_count(ny, nz, nxh):
    return 4 * ny + 1 + ny + 3 * ny + 2 + ny + 1 + 3 * ny + nz + nxh + 8


def kernel(
    sizes,
    residual_hbm,
    gate_hbm,
    up_hbm,
    w_hbm,
    cot_hbm,
    outer_hbm,
    deltas_hbm,
    momentum_hbm,
    partner_hbm,
    mixed_hbm,
    grad_gate_hbm,
    grad_up_hbm,
    grad_down_hbm,
    new_outer_hbm,
    new_momentum_hbm,
    residual_v,
    gate_v,
    up_v,
    w_v,
    cot_v,
    outer_v,
    deltas_v,
    momentum_v,
    partner_s,
    hid_t,
    hid,
    act_v,
    slope_v,
    pmine,
    psend,
    precv,
    xsend,
    xrecv,
    ysend,
    yrecv,
    fsend,
    frecv,
    zbuf,
    hsend,
    hbuf,
    mixed_v,
    grad_gate_v,
    grad_up_v,
    grad_down_v,
    new_outer_v,
    new_momentum_v,
    load_sem,
    store_sem,
    send_sem,
    recv_sem,
):
    nxh, nz, ny = sizes
    far = ny // 2
    width = cot_v.shape[2]
    half, quarter = width // 2, width // 4
    ca, cb = pl.ds(0, half), pl.ds(half, half)
    q0, q1 = pl.ds(0, quarter), pl.ds(quarter, quarter)

    xh, z, y = lax.axis_index("xh"), lax.axis_index("z"), lax.axis_index("y")
    x, c = lax.axis_index("xl"), lax.axis_index("c")

    def at_y(k):
        return lax.rem(y + (k + ny), ny)

    def block(yy, xx):
        return (yy * 2 + xx) * 2 + c

    step_to = ({"y": at_y(1)}, {"y": at_y(-1)})
    sign = (1, -1)
    across = {"xl": 1 - x}
    sibling = {"c": 1 - c}

    loads = []

    def load(src, dst):
        copy = pltpu.make_async_copy(src, dst, load_sem.at[len(loads)])
        copy.start()
        loads.append(copy)
        return copy

    own = block(y, x)
    cot_in = load(cot_hbm, cot_v.at[own])
    gate_in = load(gate_hbm, gate_v)
    up_in = load(up_hbm, up_v)
    w_in = load(w_hbm, w_v)
    outer_in = load(outer_hbm, outer_v)
    deltas_in = load(deltas_hbm, deltas_v)
    momentum_in = load(momentum_hbm, momentum_v)
    partner_in = load(partner_hbm, partner_s)
    residual_in = load(residual_hbm, residual_v)

    peers = [step_to[0], step_to[1], across, sibling]
    for k in range(1, nz):
        peers.append({"z": lax.rem(z + k, nz)})
    for k in range(1, nxh):
        peers.append({"xh": lax.rem(xh + k, nxh)})
    barrier = pltpu.get_barrier_semaphore()
    for peer in peers:
        pl.semaphore_signal(barrier, inc=1, device_id=peer, device_id_type=MESH)
    gate_in.wait()
    up_in.wait()

    links = Links(send_sem, recv_sem)

    cot_in.wait()
    pl.semaphore_wait(barrier, len(peers))

    def ag_region(way, d, part, yy):
        ref = cot_v.at[block(yy, x if part == "f" else 1 - x)]
        if part == "f":
            if d < far:
                return ref
            return ref.at[:, ca if way == RIGHT else cb]
        if d < far:
            return ref.at[:, ca]
        return ref.at[:, q0 if way == RIGHT else q1]

    def ag_send(way, d, part):
        ref = ag_region(way, d, part, at_y(-sign[way] * (d - 1)))
        links.send(("ag", way, d, part), ref, ref, step_to[way])

    def ag_arrive(way, d, part):
        ref = ag_region(way, d, part, at_y(-sign[way] * d))
        links.arrive(("ag", way, d, part), ref, step_to[way])

    def hand(key, ref):
        links.send(("hand",) + key, ref, ref, sibling)

    def cross(k):
        ref = cot_v.at[block(at_y(k), x), :, cb]
        links.send(("cross", k % ny), ref, ref, across)

    def cross_arrive(k):
        ref = cot_v.at[block(at_y(k), 1 - x), :, cb]
        links.arrive(("cross", k % ny), ref, across)
        hand(("pb", k % ny), ref)

    ref = cot_v.at[own, :, ca]
    links.send(("cross_a",), ref, ref, across)
    ag_send(RIGHT, 1, "f")
    ag_send(LEFT, 1, "f")
    cross(0)
    hand(("f", 0), cot_v.at[own])

    outer_in.wait()
    deltas_in.wait()
    zbuf[z] = (0.5 * delta_rate * deltas_v[...] + 0.5 * pull_rate * outer_v[...]).astype(BF16)
    for k in range(1, nz):
        links.send(("z", k), zbuf.at[z], zbuf.at[z], {"z": lax.rem(z + k, nz)})

    gate = gate_v[...].astype(F32)
    up = up_v[...].astype(F32)
    logistic = jax.nn.sigmoid(gate)
    act = gate * logistic
    hidden = act * up
    hid_t[...] = hidden.astype(BF16)
    ff = hidden.shape[0]
    rows = hidden.T.reshape(ny, 2, 2, 8, ff)
    for cc in range(2):
        for xx in range(2):
            piece = rows[:, xx, cc].reshape(ny * 8, ff)
            hid[cc, pl.ds(xx * ny * 8, ny * 8), :] = piece.astype(BF16)
    w_in.wait()
    for part, cols in ((0, ca), (1, cb)):
        out = jnp.dot(hid[1 - c], w_v[:, cols], preferred_element_type=F32)
        psend[:, :, :, cols] = out.astype(BF16).reshape(2, ny, 8, half)
        links.send(("pair", part), psend.at[:, :, :, cols], precv.at[:, :, :, cols], sibling)

    ref = cot_v.at[block(y, 1 - x), :, ca]
    links.arrive(("cross_a",), ref, across)
    ag_send(RIGHT, 1, "p")
    ag_send(LEFT, 1, "p")
    hand(("pa", 0), ref)

    for part, cols in ((0, ca), (1, cb)):
        out = jnp.dot(hid[c], w_v[:, cols], preferred_element_type=F32)
        pmine[:, :, :, cols] = out.reshape(2, ny, 8, half)

    act_v[...] = act
    slope_v[...] = up * (logistic * (1.0 + gate * (1.0 - logistic)))

    def ag_step(d):
        for way in (RIGHT, LEFT):
            k = -sign[way] * d
            yy = at_y(k)
            ag_arrive(way, d, "f")
            if d < far:
                ag_send(way, d + 1, "f")
                cross(k)
                hand(("f", k % ny), cot_v.at[block(yy, x)])
            elif way == LEFT:
                cross(k)
                hand(("f", k % ny), cot_v.at[block(yy, x)])
            ag_arrive(way, d, "p")
            if d < far:
                ag_send(way, d + 1, "p")
                hand(("pa", k % ny), cot_v.at[block(yy, 1 - x), :, ca])
            elif way == LEFT:
                hand(("pa", k % ny), cot_v.at[block(yy, 1 - x), :, ca])

    def mine(xx, yy, cols):
        return pmine[xx, yy, :, cols] + precv[xx, yy, :, cols].astype(F32)

    def total_of(part, yy):
        if part == F_A:
            return mine(x, yy, ca)
        if part == F_B:
            return mine(x, yy, cb) + xrecv[yy].astype(F32)
        return mine(1 - x, yy, ca)

    def covered(way, part, d):
        if d < far:
            return pl.ds(0, half)
        if part == P_A:
            return q0 if way == RIGHT else q1
        return pl.ds(0, half) if (part == F_A) == (way == RIGHT) else None

    def rs_arrive(way, d, part):
        cols = covered(way, part, d)
        if cols is not None:
            links.arrive(("rs", way, d, part), yrecv.at[way, d - 1, part, :, cols], step_to[way])
        return cols

    def came(way, d, part, cols):
        got = yrecv[way, d - 1, part, :, cols].astype(F32)
        if cols.size == half:
            return got
        rest = jnp.zeros_like(got)
        return jnp.concatenate([got, rest] if cols.start == 0 else [rest, got], axis=1)

    def rs_send(way, d, part):
        cols = covered(way, part, d)
        if cols is None:
            return
        value = total_of(part, at_y(sign[way] * d))
        if d < far:
            before = rs_arrive(way, d + 1, part)
            if before is not None:
                value = value + came(way, d + 1, part, before)
        ysend[way, d - 1, part] = value.astype(BF16)
        links.send(
            ("rs", way, d, part),
            ysend.at[way, d - 1, part, :, cols],
            yrecv.at[way, d - 1, part, :, cols],
            step_to[way],
        )

    def x_send(k):
        yy = at_y(k)
        xsend[yy] = mine(1 - x, yy, cb).astype(BF16)
        links.send(("x", k % ny), xsend.at[yy], xrecv.at[yy], across)

    def x_arrive(k):
        yy = at_y(k)
        links.arrive(("x", k % ny), xrecv.at[yy], across)

    ag_step(1)

    cols = ca
    links.arrive(("pair", 0), precv.at[:, :, :, cols], sibling)
    for part in (F_A, P_A):
        for way in (RIGHT, LEFT):
            rs_send(way, far, part)
    rs_send(LEFT, far - 1, F_A)
    links.arrive(("pair", 1), precv.at[:, :, :, cb], sibling)
    order = [far]
    for d in range(far - 1, 0, -1):
        order += [d, -d]
    order.append(0)
    for k in order:
        x_send(k)

    partner_in.wait()
    for k in range(1, nz):
        src = lax.rem(z + (nz - k), nz)
        links.arrive(("z", k), zbuf.at[src], {"z": src})
    hbuf[xh] = zbuf[lax.rem(partner_s[xh * nz + z], nz)]
    for k in range(1, nxh):
        to = lax.rem(xh + k, nxh)
        hsend[k] = zbuf[lax.rem(partner_s[to * nz + z], nz)]
        links.send(("xh", k), hsend.at[k], hbuf.at[xh], {"xh": to})

    if far > 2:
        ag_step(2)
    x_arrive(far)
    rs_send(LEFT, far, F_B)
    x_arrive(far - 1)
    rs_send(RIGHT, far - 1, F_B)
    x_arrive(-(far - 1))

    cross_arrive(0)
    cross_seen = [0]

    def cross_more(d):
        for k in (d, -d):
            if k % ny not in cross_seen:
                cross_arrive(k)
                cross_seen.append(k % ny)

    rs_send(RIGHT, far - 1, F_A)
    for way in (RIGHT, LEFT):
        rs_send(way, far - 1, P_A)
    rs_send(LEFT, far - 1, F_B)
    cross_more(1)

    for d in range(far - 2, 0, -1):
        if far - d + 1 < far:
            ag_step(far - d + 1)
        for k in (d, -d):
            x_arrive(k)
        for part in (F_A, P_A, F_B):
            for way in (RIGHT, LEFT):
                rs_send(way, d, part)
        cross_more(far - d)
    ag_step(far)
    for d in range(2, far + 1):
        cross_more(d)

    momentum_in.wait()
    for k in range(1, nxh):
        src = lax.rem(xh + (nxh - k), nxh)
        links.arrive(("xh", k), hbuf.at[src], {"xh": src})
    received = hbuf[lax.div(partner_s[xh * nz + z], nz)].astype(F32)
    new_momentum = (
        decay_rate * momentum_v[...]
        + 0.5 * delta_rate * deltas_v[...]
        - 0.5 * pull_rate * outer_v[...]
        + received
    )
    new_momentum_v[...] = new_momentum
    new_outer_v[...] = outer_v[...] + new_momentum
    stores = []

    def store(src, dst):
        copy = pltpu.make_async_copy(src, dst, store_sem.at[len(stores)])
        copy.start()
        stores.append(copy)

    store(new_momentum_v, new_momentum_hbm)
    store(new_outer_v, new_outer_hbm)

    for way in (RIGHT, LEFT):
        rs_arrive(way, 1, P_A)
    value = total_of(P_A, y)
    for way in (RIGHT, LEFT):
        value = value + yrecv[way, 0, P_A].astype(F32)
    fsend[...] = value.astype(BF16)
    links.send(("last",), fsend, frecv, across)

    for k in range(ny):
        yy = at_y(k)
        theirs = (yy * 2 + x) * 2 + 1 - c
        other = (yy * 2 + 1 - x) * 2 + 1 - c
        links.arrive(("hand", "f", k), cot_v.at[theirs], sibling)
        links.arrive(("hand", "pa", k), cot_v.at[other, :, ca], sibling)
        links.arrive(("hand", "pb", k), cot_v.at[other, :, cb], sibling)

    tokens = cot_v.shape[0] * 8
    cot = cot_v[...].reshape(tokens, width)
    grad_hidden = lax.dot_general(
        w_v[...], cot, (((1,), (1,)), ((), ())), preferred_element_type=F32
    )
    grad_gate_v[...] = (grad_hidden * slope_v[...]).astype(BF16)
    grad_up_v[...] = (grad_hidden * act_v[...]).astype(BF16)
    store(grad_gate_v, grad_gate_hbm)
    store(grad_up_v, grad_up_hbm)
    for cols in (ca, cb):
        part = cot_v[:, :, cols].reshape(tokens, half)
        grad_down_v[:, cols] = jnp.dot(hid_t[...], part, preferred_element_type=F32).astype(BF16)
        store(grad_down_v.at[:, cols], grad_down_hbm.at[:, cols])

    residual_in.wait()
    x_arrive(0)
    for part, cols in ((F_A, ca), (F_B, cb)):
        value = total_of(part, y) + residual_v[:, cols].astype(F32)
        for way in (RIGHT, LEFT):
            rs_arrive(way, 1, part)
            value = value + yrecv[way, 0, part].astype(F32)
        if part == F_A:
            links.arrive(("last",), frecv, across)
            value = value + frecv[...].astype(F32)
        mixed_v[:, cols] = value.astype(BF16)
    store(mixed_v, mixed_hbm)

    links.drain()
    for copy in stores:
        copy.wait()


def fused(sizes, residual, gate_t, up_t, w, cot, outer, deltas, momentum, partner):
    nxh, nz, ny = sizes
    width = w.shape[1]
    half, far = width // 2, ny // 2
    anywhere = pl.BlockSpec(memory_space=pl.ANY)
    count = message_count(ny, nz, nxh)
    shapes = (residual, gate_t, up_t, w, outer, outer)
    slabs = (2, ny, 8, width)
    scratch = [
        pltpu.VMEM(residual.shape, BF16),
        pltpu.VMEM(gate_t.shape, BF16),
        pltpu.VMEM(gate_t.shape, BF16),
        pltpu.VMEM(w.shape, BF16),
        pltpu.VMEM((4 * ny, 8, width), BF16),
        pltpu.VMEM(outer.shape, F32),
        pltpu.VMEM(outer.shape, F32),
        pltpu.VMEM(outer.shape, F32),
        pltpu.SMEM(partner.shape, jnp.int32),
        pltpu.VMEM(gate_t.shape, BF16),
        pltpu.VMEM((2, 2 * ny * 8, gate_t.shape[0]), BF16),
        pltpu.VMEM(gate_t.shape, F32),
        pltpu.VMEM(gate_t.shape, F32),
        pltpu.VMEM(slabs, F32),
        pltpu.VMEM(slabs, BF16),
        pltpu.VMEM(slabs, BF16),
        pltpu.VMEM((ny, 8, half), BF16),
        pltpu.VMEM((ny, 8, half), BF16),
        pltpu.VMEM((2, far, 3, 8, half), BF16),
        pltpu.VMEM((2, far, 3, 8, half), BF16),
        pltpu.VMEM((8, half), BF16),
        pltpu.VMEM((8, half), BF16),
        pltpu.VMEM((nz,) + outer.shape, BF16),
        pltpu.VMEM((nxh,) + outer.shape, BF16),
        pltpu.VMEM((nxh,) + outer.shape, BF16),
        pltpu.VMEM(residual.shape, BF16),
        pltpu.VMEM(gate_t.shape, BF16),
        pltpu.VMEM(gate_t.shape, BF16),
        pltpu.VMEM(w.shape, BF16),
        pltpu.VMEM(outer.shape, F32),
        pltpu.VMEM(outer.shape, F32),
        pltpu.SemaphoreType.DMA((9,)),
        pltpu.SemaphoreType.DMA((7,)),
        pltpu.SemaphoreType.DMA((count,)),
        pltpu.SemaphoreType.DMA((count,)),
    ]
    return pl.pallas_call(
        functools.partial(kernel, sizes),
        name="layer",
        out_shape=[jax.ShapeDtypeStruct(a.shape, a.dtype) for a in shapes],
        in_specs=[anywhere] * 9,
        out_specs=[anywhere] * 6,
        scratch_shapes=scratch,
        compiler_params=pltpu.CompilerParams(
            collective_id=0, has_side_effects=True, vmem_limit_bytes=60 * 1024 * 1024
        ),
    )(residual, gate_t, up_t, w, cot, outer, deltas, momentum, partner)


def per_device(
    sizes, residual, gate_pre, up_pre, w, cotangent, outer_weights, deltas, momentum, partner
):
    flat = (outer_weights.shape[1] // 128, 128)
    mixed, grad_gate, grad_up, grad_down, new_outer, new_momentum = fused(
        sizes,
        residual[0],
        gate_pre[0].T,
        up_pre[0].T,
        w,
        cotangent[0],
        outer_weights.reshape(flat),
        deltas.reshape(flat),
        momentum.reshape(flat),
        partner,
    )
    return (
        mixed[None],
        grad_gate.T[None],
        grad_up.T[None],
        grad_down[None],
        new_outer.reshape(outer_weights.shape),
        new_momentum.reshape(outer_weights.shape),
    )


def build(devices, sizes):
    nxh, nz, ny = sizes
    torus = Mesh(devices.reshape(nxh, nz, ny, 2, 2), ISLAND + TP)
    return jax.shard_map(
        functools.partial(per_device, sizes),
        mesh=torus,
        in_specs=(
            P(ISLAND, TP, None),
            P(ISLAND, None, TP),
            P(ISLAND, None, TP),
            P(TP, None),
            P(ISLAND, TP, None),
            P(ISLAND, TP),
            P(ISLAND, TP),
            P(ISLAND, TP),
            P(),
        ),
        out_specs=(
            P(ISLAND, TP, None),
            P(ISLAND, None, TP),
            P(ISLAND, None, TP),
            P(ISLAND, TP, None),
            P(ISLAND, TP),
            P(ISLAND, TP),
        ),
        check_vma=False,
    )


def solution(mesh):
    return build(mesh.devices, (4, 8, mesh.shape["tp"] // 4))
```
